32 devices in a mesh: lat: 8 (over y, x, core), lon: 4 (over z).
Axes of the slice: x: 2, y: 2, z: 4, core: 2. Of those that a mesh axis runs over, the one named last changes fastest.
Arguments:
- current: bfloat16 [69, 256, 512], P(None, 'lat', 'lon')
- next_fields: bfloat16 [96, 256, 512], P(('lat', 'lon')), may hold values from -6 to 6
- reader_slot: int32 [69], replicated, may hold values from 0 to 95, as said below
- first_weight: bfloat16 [9, 256, 69], replicated, may hold values from -0.25 to 0.25
- first_bias: float32 [256], replicated, may hold values from -3 to 3
- second_weight: bfloat16 [9, 256, 256], replicated, may hold values from -0.125 to 0.125
- second_bias: float32 [256], replicated, may hold values from -3 to 3
Outputs:
- features: bfloat16 [256, 256, 512], P(None, 'lat', 'lon')
- next_tile: bfloat16 [69, 256, 512], P(None, 'lat', 'lon')
The draws below stay inside these ranges and needn't reach their ends.
Inputs may be any that keep to these rules, and one draw needn't show every extreme that they name: `reader_slot`: the 69 entries are different slots.
All inputs are finite; a program needn't handle non-finite values.
Results may differ from the reference program's by a relative error of at most 0.0053.
Values may be sent and summed in bfloat16 or wider, within the bound.
A program may use at most 128 MiB of HBM per device.

```python
import jax
import jax.numpy as jnp
from jax import lax

C = 69
HID = 256
LAT_DEV = 32
LON_DEV = 128
H = 256
W = 512
SLOTS = 96


def draw_current(key, part):
    keys = jax.random.split(jax.random.fold_in(key, 11), 7)
    profile = (jnp.arange(H, dtype=jnp.float32) / (H - 1))[None, :, None]
    rough = jax.random.uniform(keys[4], (C, 1, W), jnp.float32, 0.5, 1.5)
    slope = jax.random.uniform(keys[2], (C, 1, 1), jnp.float32, -2.0, 2.0)
    lat_tiles = H // LAT_DEV
    lon_tiles = W // LON_DEV
    tile_level = jax.random.normal(keys[5], (C, lat_tiles, 1, lon_tiles, 1), jnp.float32)
    tile_field = jnp.broadcast_to(tile_level, (C, lat_tiles, LAT_DEV, lon_tiles, LON_DEV)).reshape(C, H, W)
    half_level = jax.random.normal(keys[6], (C, 1, 2), jnp.float32)
    half_field = jnp.repeat(half_level, W // 2, axis=2)
    noise = jax.random.normal(keys[0], (C, H, W), jnp.float32)
    offset = jax.random.normal(keys[1], (C, 1, 1), jnp.float32)
    spread = 1.0 + 2.0 * profile
    tile_scale = 0.8
    values = offset + 3.0 * slope * profile + tile_scale * tile_field + half_field + spread * rough * noise
    return values.astype(jnp.bfloat16)


def draw_reader_slot(key, part):
    order = jax.random.permutation(jax.random.fold_in(key, 23), SLOTS)
    return order[:C].astype(jnp.int32)


def steps_of(rng, shape, shards, smallest, top_value):
    loudness = 1.0
    for dim, shards_of in shards:
        heights = jax.random.uniform(jax.random.fold_in(jax.random.fold_in(rng, 6), dim), (shards_of,), jnp.float32, smallest / len(shards), top_value / len(shards))
        loudness = loudness * jnp.repeat(jnp.exp(heights), shape[dim] // shards_of).reshape((-1,) + (1,) * (len(shape) - 1 - dim))
    return loudness


def scatter_about(own_key, dims, scale, most, cuts=(), held_as=jnp.bfloat16):
    level = steps_of(own_key, dims, cuts, -0.22, 0.18) if cuts else 1.0
    drawn = jax.random.normal(own_key, dims, jnp.float32) * scale * level
    return jnp.minimum(jnp.maximum(drawn, -most), most).astype(held_as)


def setup_inputs(seed: int = 0) -> dict:
    key_of = jax.random.split(jax.random.key(seed), 8)
    current = draw_current(jax.random.fold_in(key_of[7], 71), 0)
    next_fields = scatter_about(key_of[1], (SLOTS, H, W), 1.0, 6.0, ((0, 32),))
    reader_slot = draw_reader_slot(jax.random.fold_in(key_of[7], 71), 0)
    first_weight = scatter_about(key_of[3], (9, HID, C), (9 * C) ** -0.5, 0.25)
    first_bias = scatter_about(key_of[4], (HID,), 0.5, 3.0, (), jnp.float32)
    second_weight = scatter_about(key_of[5], (9, HID, HID), (9 * HID) ** -0.5, 0.125)
    second_bias = scatter_about(key_of[6], (HID,), 0.5, 3.0, (), jnp.float32)
    return {"current": current, "next_fields": next_fields, "reader_slot": reader_slot, "first_weight": first_weight, "first_bias": first_bias, "second_weight": second_weight, "second_bias": second_bias}


def conv_grid(field, weight):
    padded = jnp.pad(field.astype(jnp.float32), ((0, 0), (1, 1), (0, 0)))
    padded = jnp.concatenate([padded[:, :, -1:], padded, padded[:, :, :1]], axis=2)
    rows = field.shape[1]
    cols = field.shape[2]
    total = jnp.zeros((weight.shape[1], rows, cols), jnp.float32)
    for tap in range(9):
        shifted = padded[:, tap // 3:tap // 3 + rows, tap % 3:tap % 3 + cols]
        total = total + jnp.einsum('ok,khw->ohw', weight[tap].astype(jnp.float32), shifted)
    return total

def reference(current, next_fields, reader_slot, first_weight, first_bias, second_weight, second_bias):
    values = current.astype(jnp.float32)
    cells = values.shape[1] * values.shape[2]
    mean = lax.optimization_barrier(jnp.sum(values, axis=(1, 2))) / cells
    square = lax.optimization_barrier(jnp.sum(values * values, axis=(1, 2))) / cells
    scale = 1.0 / jnp.sqrt(square - mean * mean + 1e-05)
    normed = ((values - mean[:, None, None]) * scale[:, None, None]).astype(jnp.bfloat16)
    hidden = jax.nn.gelu(conv_grid(normed, first_weight) + first_bias[:, None, None], approximate=True).astype(jnp.bfloat16)
    features = (conv_grid(hidden, second_weight) + second_bias[:, None, None]).astype(jnp.bfloat16)
    next_tile = jnp.take(next_fields, reader_slot, axis=0)
    return (features, next_tile)
```

```python
import functools

import jax
import jax.numpy as jnp
from jax import lax
from jax.experimental import pallas as pl
from jax.experimental.pallas import tpu as pltpu
from jax.sharding import PartitionSpec as P

MESH = pl.DeviceIdType.MESH
F32 = jnp.float32
BF16 = jnp.bfloat16
LANES = 128
G1 = 4
G2 = 8


def twice_half_gelu(u):
    return u + u * jnp.tanh(u * (1.5957691216057308 + 0.2854179950588114 * (u * u)))


def kernel(
    dims, cur_in, nf, w1_in, b1_in, w2_in, b2_in, feat, moved,
    cur, w1, w2, b1, b2, yf, xf, parts, turned, xs, cols, csend, hcol, rsend, rrecv, en, eh,
    xn, acc1, hp, hs, acc2, w1s, w2s, stats,
    in_sem, st_send, st_recv, ha_send, ha_recv, mv_send, mv_recv, own_sem,
):
    n_lat, n_lon, chans, rows, wide, slots, hid = dims
    n = n_lat * n_lon
    cp = -(-chans // 8) * 8
    kq = xs.shape[2]
    cb = rsend.shape[2]
    pitch = xf.shape[1]
    xflat = xf.reshape(cp * pitch, wide)
    yflat = yf.reshape(hid * pitch, wide)
    lat = lax.axis_index("lat")
    lon = lax.axis_index("lon")
    me = lat * n_lon + lon

    loads = [
        pltpu.make_async_copy(src, dst, in_sem.at[i])
        for i, (src, dst) in enumerate(((cur_in, cur), (w1_in, w1), (w2_in, w2), (b1_in, b1), (b2_in, b2)))
    ]
    for load in loads:
        load.start()

    barrier = pltpu.get_barrier_semaphore()

    def greet(d, carry):
        t = lax.rem(me + d, n)
        pl.semaphore_signal(
            barrier, inc=1, device_id=(t // n_lon, lax.rem(t, n_lon)), device_id_type=MESH
        )
        return carry

    lax.fori_loop(1, n, greet, 0)

    loads[0].wait()
    x = cur[...].astype(F32)
    xf[0:chans, 0:rows, :] = x
    by = x.reshape(chans, rows // 8, 8, wide)
    parts[0, 0 : chans * 8, :] = jnp.sum(by, axis=1).reshape(chans * 8, wide)
    parts[1, 0 : chans * 8, :] = jnp.sum(by * by, axis=1).reshape(chans * 8, wide)
    if cp > chans:
        xf[chans:cp, :, :] = jnp.zeros((cp - chans, pitch, wide), F32)
        for k in range(2):
            parts[k, chans * 8 : cp * 8, :] = jnp.zeros(((cp - chans) * 8, wide), F32)
    for k in range(2):
        s = parts[k, pl.ds(0, cp, stride=8), :]
        for j in range(1, 8):
            s = s + parts[k, pl.ds(j, cp, stride=8), :]
        s = jnp.concatenate([s, jnp.zeros((LANES - cp, wide), F32)], axis=0).T
        stats[pl.ds(me, 1), k : k + 1, :] = jnp.sum(s, axis=0, keepdims=True)[None]

    def raw_row(r):
        return xflat[pl.ds(r, cp, stride=pitch), :]

    for side, r in ((0, 0), (1, rows - 2)):
        for j in range(2):
            a = jnp.concatenate([raw_row(r + j), jnp.zeros((cb - cp, wide), F32)], axis=0)
            rsend[side, j] = a.astype(BF16)

    group = lax.broadcasted_iota(jnp.int32, (1, wide), 1) // 4
    per = wide // 4
    for base in range(0, rows, per):
        strip = jnp.zeros((cp, wide), F32)
        for r in range(min(per, rows - base)):
            strip = jnp.where(group == r, pltpu.roll(raw_row(base + r), 4 * r + 2, 1), strip)
        turned[...] = jnp.concatenate([strip, jnp.zeros((LANES - cp, wide), F32)], axis=0).T
        part = min(per, rows - base)
        e0, e1, w0, w1_ = [turned[pl.ds(c, part, stride=4), :][:, 0:cp] for c in range(4)]
        blank = jnp.zeros((part, kq - 3 * cp), F32)
        cols[0, base : base + part] = jnp.concatenate([e1, w0, w1_, blank], axis=1)
        cols[1, base : base + part] = jnp.concatenate([e0, e1, w0, blank], axis=1)
    for side in range(2):
        csend[side] = cols[side].astype(BF16)

    pl.semaphore_wait(barrier, n - 1)

    def stat_copy(d):
        t = lax.rem(me + d, n)
        return pltpu.make_async_remote_copy(
            src_ref=stats.at[me], dst_ref=stats.at[me],
            send_sem=st_send, recv_sem=st_recv,
            device_id=(t // n_lon, lax.rem(t, n_lon)), device_id_type=MESH,
        )

    def stat_start(d, carry):
        stat_copy(d).start()
        return carry


    lax.fori_loop(1, n, stat_start, 0)

    north, south = lax.rem(lat + n_lat - 1, n_lat), lax.rem(lat + 1, n_lat)
    west, east = lax.rem(lon + n_lon - 1, n_lon), lax.rem(lon + 1, n_lon)
    halos = [
        (rsend.at[0], rrecv.at[1], (north, lon)),
        (rsend.at[1], rrecv.at[0], (south, lon)),
    ]
    for side, col_to in ((0, west), (1, east)):
        into = 1 - side
        halos.append((csend.at[side], hcol.at[into, pl.ds(16, rows)], (lat, col_to)))
        halos.append((csend.at[side, pl.ds(0, 16)], hcol.at[into, pl.ds(16 + rows, 16)], (north, col_to)))
        halos.append((csend.at[side, pl.ds(rows - 16, 16)], hcol.at[into, pl.ds(0, 16)], (south, col_to)))
    copies = [
        pltpu.make_async_remote_copy(
            src_ref=src, dst_ref=dst, send_sem=ha_send.at[i], recv_sem=ha_recv.at[i],
            device_id=where, device_id_type=MESH,
        )
        for i, (src, dst, where) in enumerate(halos)
    ]
    for copy in copies:
        copy.start()


    half = max(n_lon // 2, 1)

    def field_start(i, carry):
        j = i // n_lat
        if n_lon % 2 == 0:
            mine = lon // half
            far = (1 - mine) * half + j
            near = mine * half + lax.rem(lax.rem(lon, half) + j - half + 1, half)
            tn = jnp.where(j < half, far, near)
        else:
            tn = lax.rem(lon + 1 + j, n_lon)
        k = lax.rem(i, n_lat) + jnp.where(j == n_lon - 1, 1, 0)
        tl = lax.rem(lat + k, n_lat)
        pltpu.make_async_remote_copy(
            src_ref=nf.at[:, pl.ds(pl.multiple_of(tl * rows, rows), rows), pl.ds(pl.multiple_of(tn * wide, wide), wide)],
            dst_ref=moved.at[pl.ds(me * slots, slots)],
            send_sem=mv_send, recv_sem=mv_recv,
            device_id=(tl, tn), device_id_type=MESH,
        ).start()
        return carry


    cuts = [min(e, n - 1) for e in (0, 0, 4, 8)] + [n - 1]
    lax.fori_loop(0, cuts[1], field_start, 0)
    own = pltpu.make_async_copy(
        nf.at[:, pl.ds(pl.multiple_of(lat * rows, rows), rows), pl.ds(pl.multiple_of(lon * wide, wide), wide)],
        moved.at[pl.ds(me * slots, slots)],
        own_sem,
    )
    own.start()

    def turn(a, p):
        lo = pltpu.roll(a, 1, 1)
        hi = pltpu.roll(a, wide - 1, 1)
        stacked = jnp.concatenate([lo, a, hi, jnp.zeros((kq - 3 * cp, wide), F32)], axis=0)
        xs[p] = stacked.astype(BF16).T

    def turn_row(r, carry):
        turn(raw_row(r), r + 2)
        return carry

    lax.fori_loop(0, rows, turn_row, 0, unroll=4)

    lax.fori_loop(cuts[1], cuts[2], field_start, 0)
    for load in loads[1:]:
        load.wait()
    for a in range(3):
        pieces = []
        for j in range(3):
            pieces.append(w1[3 * a + j].astype(F32))
            if cp > chans:
                pieces.append(jnp.zeros((cp - chans, hid), F32))
        pieces.append(jnp.zeros((kq - 3 * cp, hid), F32))
        w1s[pl.ds(a * kq, kq), :] = (0.5 * jnp.concatenate(pieces, axis=0)).astype(BF16)

    def turn_weight(tap, carry):
        w2s[pl.ds(pl.multiple_of(tap * hid, hid), hid), :] = w2[tap].T
        return carry

    lax.fori_loop(0, 9, turn_weight, 0)

    lax.fori_loop(cuts[2], cuts[3], field_start, 0)
    for copy in copies:
        copy.wait_recv()
    lax.fori_loop(cuts[3], cuts[4], field_start, 0)
    tall = rows + 4
    step = en.shape[1]
    for side, p in ((0, 0), (1, rows + 2)):
        for j in range(2):
            turn(rrecv[side, j].astype(F32)[0:cp], p + j)

    lane = lax.broadcasted_iota(jnp.int32, (1, kq), 1)
    for side in range(2):
        far = hcol[side].astype(F32)[14 : 14 + tall]
        mine = jnp.concatenate(
            [
                xs[p, (wide - 16 if side == 0 else 0) : (wide if side == 0 else 16), :].astype(F32)[(15 if side == 0 else 0) : (16 if side == 0 else 1)]
                for p in (0, 1)
            ]
            + [cols[1 - side]]
            + [
                xs[p, (wide - 16 if side == 0 else 0) : (wide if side == 0 else 16), :].astype(F32)[(15 if side == 0 else 0) : (16 if side == 0 else 1)]
                for p in (rows + 2, rows + 3)
            ],
            axis=0,
        )
        theirs = lane < 2 * cp if side == 0 else lane >= cp
        en[side, 0:tall, :] = jnp.where(theirs, far, mine)
        en[2 + side, 0:tall, :] = pltpu.roll(far, kq - cp if side == 0 else cp, 1)

    def patch(p, carry):
        first = xs[p, 0:16, :].astype(F32)
        spot = lax.broadcasted_iota(jnp.int32, (16, 1), 0)
        xs[p, 0:16, :] = jnp.where((spot == 0) & (lane < cp), en[2, pl.ds(p, 1), :], first).astype(BF16)
        last = xs[p, wide - 16 : wide, :].astype(F32)
        xs[p, wide - 16 : wide, :] = jnp.where(
            (spot == 15) & (lane >= 2 * cp) & (lane < 3 * cp), en[3, pl.ds(p, 1), :], last
        ).astype(BF16)
        return carry

    lax.fori_loop(0, tall, patch, 0)

    many = pltpu.make_async_copy(stats.at[pl.ds(0, n - 1)], stats.at[pl.ds(0, n - 1)], st_recv)
    many.wait()
    sums = jnp.sum(stats[...], axis=0)
    cells = n * rows * wide
    mean = sums[0:1] / cells
    scale = 1.0 / jnp.sqrt(sums[1:2] / cells - mean * mean + 1e-05)

    def thrice(v):
        v = v[:, 0:cp]
        return jnp.concatenate([v, v, v, jnp.zeros((1, kq - 3 * cp), F32)], axis=1)

    mean3 = thrice(mean)
    scale3 = thrice(scale)

    def normal(p, carry):
        xn[p] = ((xs[p].astype(F32) - mean3) * scale3).astype(BF16)
        return carry

    lax.fori_loop(0, tall, normal, 0, unroll=2)

    @pl.when(lat == 0)
    def _():
        xn[0:2] = jnp.zeros((2, wide, kq), BF16)

    @pl.when(lat == n_lat - 1)
    def _():
        xn[rows + 2 : rows + 4] = jnp.zeros((2, wide, kq), BF16)

    first = jnp.where(lat == 0, 0, -2)
    last = jnp.where(lat == n_lat - 1, rows - 1, rows + 1)
    line = lax.broadcasted_iota(jnp.int32, (step, 1), 0) - 2
    inside = (line >= first) & (line <= last)
    bias1 = 0.5 * b1[...]
    bias2 = b2[...]
    edge = jnp.concatenate(
        [jnp.where(inside, (en[side] - mean3) * scale3, 0.0) for side in range(2)], axis=0
    ).astype(BF16)
    z = [jnp.dot(edge, w1s[pl.ds(a * kq, kq), :], preferred_element_type=F32) for a in range(3)]
    for side in range(2):
        at = side * step
        h = z[0][at : at + rows + 2] + z[1][at + 1 : at + rows + 3] + z[2][at + 2 : at + rows + 4] + bias1
        eh[side, pl.ds(0, rows + 2), :] = twice_half_gelu(h)

    def conv1(q, g):
        left = jnp.concatenate([xn[pl.ds(q + a, g)].reshape(g * wide, kq) for a in range(3)], axis=1)
        acc1[0 : g * wide] = jnp.dot(left, w1s[...], preferred_element_type=F32)

    def store1(q, g):
        for k in range(g):
            hp[k, 8 : 8 + wide, :] = twice_half_gelu(acc1[k * wide : (k + 1) * wide, :] + bias1)
            hp[k, 7:8, :] = eh[0, pl.ds(q + k, 1), :]
            hp[k, 8 + wide : 9 + wide, :] = eh[1, pl.ds(q + k, 1), :]
            for m in range(3):
                hs[q + k, :, m * hid : (m + 1) * hid] = hp[k, 7 + m : 7 + m + wide, :].astype(BF16)

    def phase1(b, carry):
        store1(G1 * (b - 1), G1)
        conv1(G1 * b, G1)
        return carry

    conv1(0, G1)
    whole1 = (rows + 2) // G1
    lax.fori_loop(1, whole1, phase1, 0)
    store1(G1 * (whole1 - 1), G1)
    if (rows + 2) % G1:
        conv1(G1 * whole1, (rows + 2) % G1)
        store1(G1 * whole1, (rows + 2) % G1)

    @pl.when(lat == 0)
    def _():
        hs[0] = jnp.zeros((wide, 3 * hid), BF16)

    @pl.when(lat == n_lat - 1)
    def _():
        hs[rows + 1] = jnp.zeros((wide, 3 * hid), BF16)

    def conv2(q):
        left = jnp.concatenate([hs[pl.ds(q + a, G2)].reshape(G2 * wide, 3 * hid) for a in range(3)], axis=1)
        acc2[...] = jnp.dot(left, w2s[...], preferred_element_type=F32)

    def store2(q):
        for k in range(G2):
            yflat[pl.ds(q + k, hid, stride=pitch), :] = (acc2[k * wide : (k + 1) * wide, :] + bias2).T

    def phase2(b, carry):
        store2(G2 * (b - 1))
        conv2(G2 * b)
        return carry

    conv2(0)
    lax.fori_loop(1, rows // G2, phase2, 0)
    store2(rows - G2)

    chunk = hid // 8
    for k in range(8):
        part = pl.ds(k * chunk, chunk)
        feat[part] = yf[part, 0:rows, :].astype(BF16)

    own.wait()
    others = moved.at[pl.ds(0, (n - 1) * slots)]
    pltpu.make_async_copy(others, others, mv_recv).wait()
    pltpu.make_async_copy(others, others, mv_send).wait()
    pltpu.make_async_copy(stats.at[pl.ds(0, n - 1)], stats.at[pl.ds(0, n - 1)], st_send).wait()
    for copy in copies:
        copy.wait_send()


def give(chans, feat_in, moved, slot_in, feat, tile, slot, sems):
    want = pltpu.make_async_copy(slot_in, slot, sems.at[0])
    want.start()
    out = pltpu.make_async_copy(feat_in, feat, sems.at[1])
    out.start()
    want.wait()

    def take(c, carry):
        pltpu.make_async_copy(moved.at[slot[c]], tile.at[c], sems.at[2]).start()
        return carry

    lax.fori_loop(0, chans, take, 0)
    pltpu.make_async_copy(moved.at[pl.ds(0, chans)], tile, sems.at[2]).wait()
    out.wait()


def body(current, next_fields, reader_slot, first_weight, first_bias, second_weight, second_bias):
    n_lat, n_lon = lax.axis_size("lat"), lax.axis_size("lon")
    n = n_lat * n_lon
    chans, rows, wide = current.shape
    slots = next_fields.shape[0]
    hid = first_weight.shape[1]
    cp = -(-chans // 8) * 8
    cb = -(-chans // 16) * 16
    kq = -(-3 * cp // LANES) * LANES
    pitch = 8 * (rows // 8 + 1 - rows // 8 % 2)
    step = -(-(rows + 4) // 16) * 16
    dims = (n_lat, n_lon, chans, rows, wide, slots, hid)
    vmem = pl.BlockSpec(memory_space=pltpu.VMEM)
    hbm = pl.BlockSpec(memory_space=pltpu.HBM)
    hold = pltpu.with_memory_space_constraint
    made, moved = pl.pallas_call(
        functools.partial(kernel, dims),
        out_shape=(
            jax.ShapeDtypeStruct((hid, rows, wide), BF16),
            jax.ShapeDtypeStruct((n * slots, rows, wide), BF16),
        ),
        in_specs=[hbm] * 6,
        out_specs=(vmem, vmem),
        scratch_shapes=[
            pltpu.VMEM((chans, rows, wide), BF16),
            pltpu.VMEM((9, chans, hid), BF16),
            pltpu.VMEM((9, hid, hid), BF16),
            pltpu.VMEM((1, hid), F32),
            pltpu.VMEM((1, hid), F32),
            pltpu.VMEM((hid, pitch, wide), F32),
            pltpu.VMEM((cp, pitch, wide), F32),
            pltpu.VMEM((2, cp * 8, wide), F32),
            pltpu.VMEM((wide, LANES), F32),
            pltpu.VMEM((rows + 4, wide, kq), BF16),
            pltpu.VMEM((2, rows, kq), F32),
            pltpu.VMEM((2, rows, kq), BF16),
            pltpu.VMEM((2, rows + 32, kq), BF16),
            pltpu.VMEM((2, 2, cb, wide), BF16),
            pltpu.VMEM((2, 2, cb, wide), BF16),
            pltpu.VMEM((4, step, kq), F32),
            pltpu.VMEM((2, step, hid), F32),
            pltpu.VMEM((rows + 4, wide, kq), BF16),
            pltpu.VMEM((G1 * wide, hid), F32),
            pltpu.VMEM((G1, wide + 16, hid), F32),
            pltpu.VMEM((rows + 2, wide, 3 * hid), BF16),
            pltpu.VMEM((G2 * wide, hid), F32),
            pltpu.VMEM((3 * kq, hid), BF16),
            pltpu.VMEM((9 * hid, hid), BF16),
            pltpu.VMEM((n, 2, LANES), F32),
            pltpu.SemaphoreType.DMA((5,)),
            pltpu.SemaphoreType.DMA,
            pltpu.SemaphoreType.DMA,
            pltpu.SemaphoreType.DMA((8,)),
            pltpu.SemaphoreType.DMA((8,)),
            pltpu.SemaphoreType.DMA,
            pltpu.SemaphoreType.DMA,
            pltpu.SemaphoreType.DMA,
        ],
        compiler_params=pltpu.CompilerParams(
            collective_id=0, has_side_effects=True, vmem_limit_bytes=40 * 1024 * 1024
        ),
    )(
        *[
            hold(x, pltpu.HBM)
            for x in (
                current, next_fields, first_weight.transpose(0, 2, 1),
                first_bias[None], second_weight, second_bias[None],
            )
        ]
    )
    return pl.pallas_call(
        functools.partial(give, chans),
        out_shape=(
            jax.ShapeDtypeStruct((hid, rows, wide), BF16),
            jax.ShapeDtypeStruct((chans, rows, wide), BF16),
        ),
        in_specs=[vmem, vmem, hbm],
        out_specs=(hbm, hbm),
        scratch_shapes=[pltpu.SMEM((chans,), jnp.int32), pltpu.SemaphoreType.DMA((3,))],
        compiler_params=pltpu.CompilerParams(vmem_limit_bytes=8 * 1024 * 1024),
    )(made, moved, hold(reader_slot, pltpu.HBM))


def solution(mesh):
    in_specs = (P(None, "lat", "lon"), P(("lat", "lon"), None, None), P(), P(), P(), P(), P())
    out_specs = (P(None, "lat", "lon"), P(None, "lat", "lon"))
    return jax.shard_map(body, mesh=mesh, in_specs=in_specs, out_specs=out_specs, check_vma=False)
```

```python
import functools

import jax
import jax.numpy as jnp
from jax import lax
from jax.experimental import pallas as pl
from jax.experimental.pallas import tpu as pltpu
from jax.sharding import PartitionSpec as P

MESH = pl.DeviceIdType.MESH
F32 = jnp.float32
BF16 = jnp.bfloat16
LANES = 128
NEAR = 4
OUTER = 0
INNER = 6
G1 = 4
G2 = 8


def twice_half_gelu(u):
    return u + u * jnp.tanh(u * (1.5957691216057308 + 0.2854179950588114 * (u * u)))


def kernel(
    dims, cur_in, nf, w1_in, b1_in, w2_in, b2_in, feat, moved,
    cur, w1, w2, b1, b2, yf, xf, parts, turned, xs, cols, csend, hcol, ksend, krecv, rsend, rrecv, en, eh,
    xn, acc1, hp, hs, acc2, w1s, w2s, stats,
    in_sem, st_send, st_recv, ha_send, ha_recv, mv_send, mv_recv, own_sem,
):
    n_lat, n_lon, chans, rows, wide, slots, hid = dims
    n = n_lat * n_lon
    cp = -(-chans // 8) * 8
    kq = xs.shape[2]
    cb = rsend.shape[2]
    pitch = xf.shape[1]
    xflat = xf.reshape(cp * pitch, wide)
    yflat = yf.reshape(hid * pitch, wide)
    lat = lax.axis_index("lat")
    lon = lax.axis_index("lon")
    me = lat * n_lon + lon

    loads = [
        pltpu.make_async_copy(src, dst, in_sem.at[i])
        for i, (src, dst) in enumerate(((cur_in, cur), (w1_in, w1), (w2_in, w2), (b1_in, b1), (b2_in, b2)))
    ]
    for load in loads:
        load.start()

    barrier = pltpu.get_barrier_semaphore()

    def everyone(act):
        across = [lax.rem(lon + b, n_lon) for b in range(n_lon)]
        for b in range(1, n_lon):
            act((lat, across[b]))

        def along(a, carry):
            tl = lax.rem(lat + a, n_lat)
            for b in range(n_lon):
                act((tl, across[b]))
            return carry

        lax.fori_loop(1, n_lat, along, 0)

    everyone(
        lambda t: pl.semaphore_signal(barrier, inc=1, device_id=t, device_id_type=MESH)
    )

    loads[0].wait()
    x = cur[...].astype(F32)
    xf[0:chans, 0:rows, :] = x
    by = x.reshape(chans, rows // 8, 8, wide)
    parts[0, 0 : chans * 8, :] = jnp.sum(by, axis=1).reshape(chans * 8, wide)
    parts[1, 0 : chans * 8, :] = jnp.sum(by * by, axis=1).reshape(chans * 8, wide)
    if cp > chans:
        xf[chans:cp, :, :] = jnp.zeros((cp - chans, pitch, wide), F32)
        for k in range(2):
            parts[k, chans * 8 : cp * 8, :] = jnp.zeros(((cp - chans) * 8, wide), F32)
    for k in range(2):
        s = parts[k, pl.ds(0, cp, stride=8), :]
        for j in range(1, 8):
            s = s + parts[k, pl.ds(j, cp, stride=8), :]
        s = jnp.concatenate([s, jnp.zeros((LANES - cp, wide), F32)], axis=0).T
        stats[pl.ds(me, 1), k : k + 1, :] = jnp.sum(s, axis=0, keepdims=True)[None]

    def raw_row(r):
        return xflat[pl.ds(r, cp, stride=pitch), :]

    for side, r in ((0, 0), (1, rows - 2)):
        for j in range(2):
            a = jnp.concatenate([raw_row(r + j), jnp.zeros((cb - cp, wide), F32)], axis=0)
            rsend[side, j] = a.astype(BF16)

    group = lax.broadcasted_iota(jnp.int32, (1, wide), 1) // 4
    per = wide // 4
    for base in range(0, rows, per):
        strip = jnp.zeros((cp, wide), F32)
        for r in range(min(per, rows - base)):
            strip = jnp.where(group == r, pltpu.roll(raw_row(base + r), 4 * r + 2, 1), strip)
        turned[...] = jnp.concatenate([strip, jnp.zeros((LANES - cp, wide), F32)], axis=0).T
        part = min(per, rows - base)
        e0, e1, w0, w1_ = [turned[pl.ds(c, part, stride=4), :][:, 0:cp] for c in range(4)]
        blank = jnp.zeros((part, kq - 3 * cp), F32)
        cols[0, base : base + part] = jnp.concatenate([e1, w0, w1_, blank], axis=1)
        cols[1, base : base + part] = jnp.concatenate([e0, e1, w0, blank], axis=1)
    for side in range(2):
        csend[side] = cols[side].astype(BF16)
        ksend[2 * side] = cols[side, 0:2]
        ksend[2 * side + 1] = cols[side, rows - 2 : rows]

    pl.semaphore_wait(barrier, n - 1)

    everyone(
        lambda t: pltpu.make_async_remote_copy(
            src_ref=stats.at[me], dst_ref=stats.at[me], send_sem=st_send, recv_sem=st_recv,
            device_id=t, device_id_type=MESH,
        ).start()
    )

    north, south = lax.rem(lat + n_lat - 1, n_lat), lax.rem(lat + 1, n_lat)
    west, east = lax.rem(lon + n_lon - 1, n_lon), lax.rem(lon + 1, n_lon)
    above, below = lat > 0, lat < n_lat - 1
    halos = []
    for side, col_to in ((0, west), (1, east)):
        into = 1 - side
        halos.append((csend.at[side], hcol.at[into], (lat, col_to), None, None))
        halos.append((ksend.at[2 * side], krecv.at[2 * into + 1], (north, col_to), above, below))
        halos.append((ksend.at[2 * side + 1], krecv.at[2 * into], (south, col_to), below, above))
    halos.append((rsend.at[0], rrecv.at[1], (north, lon), above, below))
    halos.append((rsend.at[1], rrecv.at[0], (south, lon), below, above))
    copies = [
        (
            pltpu.make_async_remote_copy(
                src_ref=src, dst_ref=dst, send_sem=ha_send.at[i], recv_sem=ha_recv.at[i],
                device_id=where, device_id_type=MESH,
            ),
            sends, gets,
        )
        for i, (src, dst, where, sends, gets) in enumerate(halos)
    ]

    def each(act, which):
        for entry in copies:
            if entry[which] is None:
                act(entry[0])
            else:
                pl.when(entry[which])(functools.partial(act, entry[0]))

    each(lambda copy: copy.start(), 1)

    half = max(n_lon // 2, 1)

    if n_lon % 2 == 0:
        mine, place = lon // half, lax.rem(lon, half)
        outer = jnp.where(mine == 0, place < half - half // 2, place >= half // 2)
    else:
        outer = lon < 0

    once = (half - 1) * n_lat

    def field_start(i, carry):
        if n_lon % 2 == 0:
            f = i - once
            turned_f = jnp.where(f < NEAR, once + f, jnp.where(f < NEAR + once, f - NEAR, f))
            f = jnp.where(outer | (mine == 0), f, turned_f)
            f = jnp.where(f < 0, 0, f)
            is_near, is_own = i < once, i >= (n_lon - 1) * n_lat
            tn = jnp.where(is_near, mine * half + lax.rem(place + i // n_lat + 1, half), (1 - mine) * half + f // n_lat)
            tn = jnp.where(is_own, lon, tn)
            k = lax.rem(jnp.where(is_near | is_own, i, f), n_lat) + jnp.where(is_own, 1, 0)
        else:
            j = i // n_lat
            tn = lax.rem(lon + 1 + j, n_lon)
            k = lax.rem(i, n_lat) + jnp.where(j == n_lon - 1, 1, 0)
        tl = lax.rem(lat + k, n_lat)
        pltpu.make_async_remote_copy(
            src_ref=nf.at[:, pl.ds(pl.multiple_of(tl * rows, rows), rows), pl.ds(pl.multiple_of(tn * wide, wide), wide)],
            dst_ref=moved.at[pl.ds(me * slots, slots)],
            send_sem=mv_send, recv_sem=mv_recv,
            device_id=(tl, tn), device_id_type=MESH,
        ).start()
        return carry


    cut1 = jnp.where(outer, once + OUTER, once + INNER)
    lax.fori_loop(0, cut1, field_start, 0)
    own = pltpu.make_async_copy(
        nf.at[:, pl.ds(pl.multiple_of(lat * rows, rows), rows), pl.ds(pl.multiple_of(lon * wide, wide), wide)],
        moved.at[pl.ds(me * slots, slots)],
        own_sem,
    )
    own.start()

    def turn(a, p):
        lo = pltpu.roll(a, 1, 1)
        hi = pltpu.roll(a, wide - 1, 1)
        stacked = jnp.concatenate([lo, a, hi, jnp.zeros((kq - 3 * cp, wide), F32)], axis=0)
        xs[p] = stacked.astype(BF16).T

    def turn_row(r, carry):
        turn(raw_row(r), r + 2)
        return carry

    lax.fori_loop(0, rows, turn_row, 0, unroll=4)

    for load in loads[1:]:
        load.wait()
    for a in range(3):
        pieces = []
        for j in range(3):
            pieces.append(w1[3 * a + j].astype(F32))
            if cp > chans:
                pieces.append(jnp.zeros((cp - chans, hid), F32))
        pieces.append(jnp.zeros((kq - 3 * cp, hid), F32))
        w1s[pl.ds(a * kq, kq), :] = (0.5 * jnp.concatenate(pieces, axis=0)).astype(BF16)

    def turn_weight(tap, carry):
        w2s[pl.ds(pl.multiple_of(tap * hid, hid), hid), :] = w2[tap].T
        return carry

    lax.fori_loop(0, 9, turn_weight, 0)

    each(lambda copy: copy.wait_recv(), 2)
    lax.fori_loop(cut1, n - 1, field_start, 0)
    tall = rows + 4
    step = en.shape[1]
    for side, p in ((0, 0), (1, rows + 2)):
        for j in range(2):
            turn(rrecv[side, j].astype(F32)[0:cp], p + j)

    lane = lax.broadcasted_iota(jnp.int32, (1, kq), 1)
    for side in range(2):
        far = jnp.concatenate([krecv[2 * side], hcol[side].astype(F32), krecv[2 * side + 1]], axis=0)
        mine = jnp.concatenate(
            [
                xs[p, (wide - 16 if side == 0 else 0) : (wide if side == 0 else 16), :].astype(F32)[(15 if side == 0 else 0) : (16 if side == 0 else 1)]
                for p in (0, 1)
            ]
            + [cols[1 - side]]
            + [
                xs[p, (wide - 16 if side == 0 else 0) : (wide if side == 0 else 16), :].astype(F32)[(15 if side == 0 else 0) : (16 if side == 0 else 1)]
                for p in (rows + 2, rows + 3)
            ],
            axis=0,
        )
        theirs = lane < 2 * cp if side == 0 else lane >= cp
        en[side, 0:tall, :] = jnp.where(theirs, far, mine)
        en[2 + side, 0:tall, :] = pltpu.roll(far, kq - cp if side == 0 else cp, 1)

    def patch(p, carry):
        first = xs[p, 0:16, :].astype(F32)
        spot = lax.broadcasted_iota(jnp.int32, (16, 1), 0)
        xs[p, 0:16, :] = jnp.where((spot == 0) & (lane < cp), en[2, pl.ds(p, 1), :], first).astype(BF16)
        last = xs[p, wide - 16 : wide, :].astype(F32)
        xs[p, wide - 16 : wide, :] = jnp.where(
            (spot == 15) & (lane >= 2 * cp) & (lane < 3 * cp), en[3, pl.ds(p, 1), :], last
        ).astype(BF16)
        return carry

    lax.fori_loop(0, tall, patch, 0)

    many = pltpu.make_async_copy(stats.at[pl.ds(0, n - 1)], stats.at[pl.ds(0, n - 1)], st_recv)
    many.wait()
    sums = jnp.sum(stats[...], axis=0)
    cells = n * rows * wide
    mean = sums[0:1] / cells
    scale = 1.0 / jnp.sqrt(sums[1:2] / cells - mean * mean + 1e-05)

    def thrice(v):
        v = v[:, 0:cp]
        return jnp.concatenate([v, v, v, jnp.zeros((1, kq - 3 * cp), F32)], axis=1)

    mean3 = thrice(mean)
    scale3 = thrice(scale)

    def normal(p, carry):
        xn[p] = ((xs[p].astype(F32) - mean3) * scale3).astype(BF16)
        return carry

    lax.fori_loop(0, tall, normal, 0, unroll=2)

    @pl.when(lat == 0)
    def _():
        xn[0:2] = jnp.zeros((2, wide, kq), BF16)

    @pl.when(lat == n_lat - 1)
    def _():
        xn[rows + 2 : rows + 4] = jnp.zeros((2, wide, kq), BF16)

    first = jnp.where(lat == 0, 0, -2)
    last = jnp.where(lat == n_lat - 1, rows - 1, rows + 1)
    line = lax.broadcasted_iota(jnp.int32, (step, 1), 0) - 2
    inside = (line >= first) & (line <= last)
    bias1 = 0.5 * b1[...]
    bias2 = b2[...]
    edge = jnp.concatenate(
        [jnp.where(inside, (en[side] - mean3) * scale3, 0.0) for side in range(2)], axis=0
    ).astype(BF16)
    z = [jnp.dot(edge, w1s[pl.ds(a * kq, kq), :], preferred_element_type=F32) for a in range(3)]
    for side in range(2):
        at = side * step
        h = z[0][at : at + rows + 2] + z[1][at + 1 : at + rows + 3] + z[2][at + 2 : at + rows + 4] + bias1
        eh[side, pl.ds(0, rows + 2), :] = twice_half_gelu(h)

    def conv1(q, g):
        left = jnp.concatenate([xn[pl.ds(q + a, g)].reshape(g * wide, kq) for a in range(3)], axis=1)
        acc1[0 : g * wide] = jnp.dot(left, w1s[...], preferred_element_type=F32)

    def store1(q, g):
        for k in range(g):
            hp[k, 8 : 8 + wide, :] = twice_half_gelu(acc1[k * wide : (k + 1) * wide, :] + bias1)
            hp[k, 7:8, :] = eh[0, pl.ds(q + k, 1), :]
            hp[k, 8 + wide : 9 + wide, :] = eh[1, pl.ds(q + k, 1), :]
            for m in range(3):
                hs[q + k, :, m * hid : (m + 1) * hid] = hp[k, 7 + m : 7 + m + wide, :].astype(BF16)

    def phase1(b, carry):
        store1(G1 * (b - 1), G1)
        conv1(G1 * b, G1)
        return carry

    conv1(0, G1)
    whole1 = (rows + 2) // G1
    lax.fori_loop(1, whole1, phase1, 0)
    store1(G1 * (whole1 - 1), G1)
    if (rows + 2) % G1:
        conv1(G1 * whole1, (rows + 2) % G1)
        store1(G1 * whole1, (rows + 2) % G1)

    @pl.when(lat == 0)
    def _():
        hs[0] = jnp.zeros((wide, 3 * hid), BF16)

    @pl.when(lat == n_lat - 1)
    def _():
        hs[rows + 1] = jnp.zeros((wide, 3 * hid), BF16)

    def conv2(q):
        left = jnp.concatenate([hs[pl.ds(q + a, G2)].reshape(G2 * wide, 3 * hid) for a in range(3)], axis=1)
        acc2[...] = jnp.dot(left, w2s[...], preferred_element_type=F32)

    def store2(q):
        for k in range(G2):
            yflat[pl.ds(q + k, hid, stride=pitch), :] = (acc2[k * wide : (k + 1) * wide, :] + bias2).T

    def phase2(b, carry):
        store2(G2 * (b - 1))
        conv2(G2 * b)
        return carry

    conv2(0)
    lax.fori_loop(1, rows // G2, phase2, 0)
    store2(rows - G2)

    chunk = hid // 8
    for k in range(8):
        part = pl.ds(k * chunk, chunk)
        feat[part] = yf[part, 0:rows, :].astype(BF16)

    own.wait()
    others = moved.at[pl.ds(0, (n - 1) * slots)]
    pltpu.make_async_copy(others, others, mv_recv).wait()
    pltpu.make_async_copy(others, others, mv_send).wait()
    pltpu.make_async_copy(stats.at[pl.ds(0, n - 1)], stats.at[pl.ds(0, n - 1)], st_send).wait()
    each(lambda copy: copy.wait_send(), 1)


def give(chans, feat_in, moved, slot_in, feat, tile, slot, sems):
    want = pltpu.make_async_copy(slot_in, slot, sems.at[0])
    want.start()
    out = pltpu.make_async_copy(feat_in, feat, sems.at[1])
    out.start()
    want.wait()

    for c in range(chans):
        pltpu.make_async_copy(moved.at[slot[c]], tile.at[c], sems.at[2]).start()
    pltpu.make_async_copy(moved.at[pl.ds(0, chans)], tile, sems.at[2]).wait()
    out.wait()


def body(current, next_fields, reader_slot, first_weight, first_bias, second_weight, second_bias):
    n_lat, n_lon = lax.axis_size("lat"), lax.axis_size("lon")
    n = n_lat * n_lon
    chans, rows, wide = current.shape
    slots = next_fields.shape[0]
    hid = first_weight.shape[1]
    cp = -(-chans // 8) * 8
    cb = -(-chans // 16) * 16
    kq = -(-3 * cp // LANES) * LANES
    pitch = 8 * (rows // 8 + 1 - rows // 8 % 2)
    step = -(-(rows + 4) // 16) * 16
    dims = (n_lat, n_lon, chans, rows, wide, slots, hid)
    vmem = pl.BlockSpec(memory_space=pltpu.VMEM)
    hbm = pl.BlockSpec(memory_space=pltpu.HBM)
    hold = pltpu.with_memory_space_constraint
    made, moved = pl.pallas_call(
        functools.partial(kernel, dims),
        out_shape=(
            jax.ShapeDtypeStruct((hid, rows, wide), BF16),
            jax.ShapeDtypeStruct((n * slots, rows, wide), BF16),
        ),
        in_specs=[hbm] * 6,
        out_specs=(vmem, vmem),
        scratch_shapes=[
            pltpu.VMEM((chans, rows, wide), BF16),
            pltpu.VMEM((9, chans, hid), BF16),
            pltpu.VMEM((9, hid, hid), BF16),
            pltpu.VMEM((1, hid), F32),
            pltpu.VMEM((1, hid), F32),
            pltpu.VMEM((hid, pitch, wide), F32),
            pltpu.VMEM((cp, pitch, wide), F32),
            pltpu.VMEM((2, cp * 8, wide), F32),
            pltpu.VMEM((wide, LANES), F32),
            pltpu.VMEM((rows + 4, wide, kq), BF16),
            pltpu.VMEM((2, rows, kq), F32),
            pltpu.VMEM((2, rows, kq), BF16),
            pltpu.VMEM((2, rows, kq), BF16),
            pltpu.VMEM((4, 2, kq), F32),
            pltpu.VMEM((4, 2, kq), F32),
            pltpu.VMEM((2, 2, cb, wide), BF16),
            pltpu.VMEM((2, 2, cb, wide), BF16),
            pltpu.VMEM((4, step, kq), F32),
            pltpu.VMEM((2, step, hid), F32),
            pltpu.VMEM((rows + 4, wide, kq), BF16),
            pltpu.VMEM((G1 * wide, hid), F32),
            pltpu.VMEM((G1, wide + 16, hid), F32),
            pltpu.VMEM((rows + 2, wide, 3 * hid), BF16),
            pltpu.VMEM((G2 * wide, hid), F32),
            pltpu.VMEM((3 * kq, hid), BF16),
            pltpu.VMEM((9 * hid, hid), BF16),
            pltpu.VMEM((n, 2, LANES), F32),
            pltpu.SemaphoreType.DMA((5,)),
            pltpu.SemaphoreType.DMA,
            pltpu.SemaphoreType.DMA,
            pltpu.SemaphoreType.DMA((8,)),
            pltpu.SemaphoreType.DMA((8,)),
            pltpu.SemaphoreType.DMA,
            pltpu.SemaphoreType.DMA,
            pltpu.SemaphoreType.DMA,
        ],
        compiler_params=pltpu.CompilerParams(
            collective_id=0, has_side_effects=True, vmem_limit_bytes=40 * 1024 * 1024
        ),
    )(
        *[
            hold(x, pltpu.HBM)
            for x in (
                current, next_fields, first_weight.transpose(0, 2, 1),
                first_bias[None], second_weight, second_bias[None],
            )
        ]
    )
    return pl.pallas_call(
        functools.partial(give, chans),
        out_shape=(
            jax.ShapeDtypeStruct((hid, rows, wide), BF16),
            jax.ShapeDtypeStruct((chans, rows, wide), BF16),
        ),
        in_specs=[vmem, vmem, hbm],
        out_specs=(hbm, hbm),
        scratch_shapes=[pltpu.SMEM((chans,), jnp.int32), pltpu.SemaphoreType.DMA((3,))],
        compiler_params=pltpu.CompilerParams(vmem_limit_bytes=8 * 1024 * 1024),
    )(made, moved, hold(reader_slot, pltpu.HBM))


def solution(mesh):
    in_specs = (P(None, "lat", "lon"), P(("lat", "lon"), None, None), P(), P(), P(), P(), P())
    out_specs = (P(None, "lat", "lon"), P(None, "lat", "lon"))
    return jax.shard_map(body, mesh=mesh, in_specs=in_specs, out_specs=out_specs, check_vma=False)
```

```python
import functools

import jax
import jax.numpy as jnp
from jax import lax
from jax.experimental import pallas as pl
from jax.experimental.pallas import tpu as pltpu
from jax.sharding import PartitionSpec as P

MESH = pl.DeviceIdType.MESH
F32 = jnp.float32
BF16 = jnp.bfloat16
LANES = 128
PIECES = 2
NEAR = 4
OUTER = 0
INNER = 6
G1 = 4
G2 = 8


def twice_half_gelu(u):
    return u + u * jnp.tanh(u * (1.5957691216057308 + 0.2854179950588114 * (u * u)))


def kernel(
    dims, cur_in, nf, w1_in, b1_in, w2_in, b2_in, feat, moved,
    cur, w1, w2, b1, b2, yf, xf, parts, turned, xs, cols, csend, hcol, ksend, krecv, rsend, rrecv, en, eh,
    xn, acc1, hp, hs, acc2, w1s, w2s, stats,
    in_sem, st_send, st_recv, ha_send, ha_recv, mv_send, mv_recv, own_sem,
):
    n_lat, n_lon, chans, rows, wide, slots, hid = dims
    n = n_lat * n_lon
    cp = -(-chans // 8) * 8
    kq = xs.shape[2]
    cb = rsend.shape[2]
    pitch = xf.shape[1]
    xflat = xf.reshape(cp * pitch, wide)
    yflat = yf.reshape(hid * pitch, wide)
    lat = lax.axis_index("lat")
    lon = lax.axis_index("lon")
    me = lat * n_lon + lon

    loads = [
        pltpu.make_async_copy(src, dst, in_sem.at[i])
        for i, (src, dst) in enumerate(((cur_in, cur), (w1_in, w1), (w2_in, w2), (b1_in, b1), (b2_in, b2)))
    ]
    for load in loads:
        load.start()

    barrier = pltpu.get_barrier_semaphore()

    def everyone(act):
        across = [lax.rem(lon + b, n_lon) for b in range(n_lon)]
        for b in range(1, n_lon):
            act((lat, across[b]))

        def along(a, carry):
            tl = lax.rem(lat + a, n_lat)
            for b in range(n_lon):
                act((tl, across[b]))
            return carry

        lax.fori_loop(1, n_lat, along, 0)

    everyone(
        lambda t: pl.semaphore_signal(barrier, inc=1, device_id=t, device_id_type=MESH)
    )

    loads[0].wait()
    x = cur[...].astype(F32)
    xf[0:chans, 0:rows, :] = x
    by = x.reshape(chans, rows // 8, 8, wide)
    parts[0, 0 : chans * 8, :] = jnp.sum(by, axis=1).reshape(chans * 8, wide)
    parts[1, 0 : chans * 8, :] = jnp.sum(by * by, axis=1).reshape(chans * 8, wide)
    if cp > chans:
        xf[chans:cp, :, :] = jnp.zeros((cp - chans, pitch, wide), F32)
        for k in range(2):
            parts[k, chans * 8 : cp * 8, :] = jnp.zeros(((cp - chans) * 8, wide), F32)
    for k in range(2):
        s = parts[k, pl.ds(0, cp, stride=8), :]
        for j in range(1, 8):
            s = s + parts[k, pl.ds(j, cp, stride=8), :]
        s = jnp.concatenate([s, jnp.zeros((LANES - cp, wide), F32)], axis=0).T
        stats[pl.ds(me, 1), k : k + 1, :] = jnp.sum(s, axis=0, keepdims=True)[None]

    def raw_row(r):
        return xflat[pl.ds(r, cp, stride=pitch), :]

    for side, r in ((0, 0), (1, rows - 2)):
        for j in range(2):
            a = jnp.concatenate([raw_row(r + j), jnp.zeros((cb - cp, wide), F32)], axis=0)
            rsend[side, j] = a.astype(BF16)

    group = lax.broadcasted_iota(jnp.int32, (1, wide), 1) // 4
    per = wide // 4
    for base in range(0, rows, per):
        strip = jnp.zeros((cp, wide), F32)
        for r in range(min(per, rows - base)):
            strip = jnp.where(group == r, pltpu.roll(raw_row(base + r), 4 * r + 2, 1), strip)
        turned[...] = jnp.concatenate([strip, jnp.zeros((LANES - cp, wide), F32)], axis=0).T
        part = min(per, rows - base)
        e0, e1, w0, w1_ = [turned[pl.ds(c, part, stride=4), :][:, 0:cp] for c in range(4)]
        blank = jnp.zeros((part, kq - 3 * cp), F32)
        cols[0, base : base + part] = jnp.concatenate([e1, w0, w1_, blank], axis=1)
        cols[1, base : base + part] = jnp.concatenate([e0, e1, w0, blank], axis=1)
    for side in range(2):
        csend[side] = cols[side].astype(BF16)
        ksend[2 * side] = cols[side, 0:2]
        ksend[2 * side + 1] = cols[side, rows - 2 : rows]

    pl.semaphore_wait(barrier, n - 1)

    everyone(
        lambda t: pltpu.make_async_remote_copy(
            src_ref=stats.at[me], dst_ref=stats.at[me], send_sem=st_send, recv_sem=st_recv,
            device_id=t, device_id_type=MESH,
        ).start()
    )

    north, south = lax.rem(lat + n_lat - 1, n_lat), lax.rem(lat + 1, n_lat)
    west, east = lax.rem(lon + n_lon - 1, n_lon), lax.rem(lon + 1, n_lon)
    above, below = lat > 0, lat < n_lat - 1
    halos = []
    for side, col_to in ((0, west), (1, east)):
        into = 1 - side
        halos.append((csend.at[side], hcol.at[into], (lat, col_to), None, None))
        halos.append((ksend.at[2 * side], krecv.at[2 * into + 1], (north, col_to), above, below))
        halos.append((ksend.at[2 * side + 1], krecv.at[2 * into], (south, col_to), below, above))
    halos.append((rsend.at[0], rrecv.at[1], (north, lon), above, below))
    halos.append((rsend.at[1], rrecv.at[0], (south, lon), below, above))
    copies = [
        (
            pltpu.make_async_remote_copy(
                src_ref=src, dst_ref=dst, send_sem=ha_send.at[i], recv_sem=ha_recv.at[i],
                device_id=where, device_id_type=MESH,
            ),
            sends, gets,
        )
        for i, (src, dst, where, sends, gets) in enumerate(halos)
    ]

    def each(act, which):
        for entry in copies:
            if entry[which] is None:
                act(entry[0])
            else:
                pl.when(entry[which])(functools.partial(act, entry[0]))

    each(lambda copy: copy.start(), 1)

    half = max(n_lon // 2, 1)

    if n_lon % 2 == 0:
        mine, place = lon // half, lax.rem(lon, half)
        outer = jnp.where(mine == 0, place < half - half // 2, place >= half // 2)
    else:
        outer = lon < 0

    once = (half - 1) * n_lat

    def field_start(i, carry):
        if n_lon % 2 == 0:
            f = i - once
            turned_f = jnp.where(f < NEAR, once + f, jnp.where(f < NEAR + once, f - NEAR, f))
            f = jnp.where(outer | (mine == 0), f, turned_f)
            f = jnp.where(f < 0, 0, f)
            is_near, is_own = i < once, i >= (n_lon - 1) * n_lat
            tn = jnp.where(is_near, mine * half + lax.rem(place + i // n_lat + 1, half), (1 - mine) * half + f // n_lat)
            tn = jnp.where(is_own, lon, tn)
            k = lax.rem(jnp.where(is_near | is_own, i, f), n_lat) + jnp.where(is_own, 1, 0)
        else:
            j = i // n_lat
            tn = lax.rem(lon + 1 + j, n_lon)
            k = lax.rem(i, n_lat) + jnp.where(j == n_lon - 1, 1, 0)
        tl = lax.rem(lat + k, n_lat)
        pltpu.make_async_remote_copy(
            src_ref=nf.at[:, pl.ds(pl.multiple_of(tl * rows, rows), rows), pl.ds(pl.multiple_of(tn * wide, wide), wide)],
            dst_ref=moved.at[pl.ds(me * slots, slots)],
            send_sem=mv_send, recv_sem=mv_recv,
            device_id=(tl, tn), device_id_type=MESH,
        ).start()
        return carry


    cut1 = jnp.where(outer, once + OUTER, once + INNER)
    lax.fori_loop(once, cut1, field_start, 0)
    lax.fori_loop(0, once, field_start, 0)
    own = pltpu.make_async_copy(
        nf.at[:, pl.ds(pl.multiple_of(lat * rows, rows), rows), pl.ds(pl.multiple_of(lon * wide, wide), wide)],
        moved.at[pl.ds(me * slots, slots)],
        own_sem,
    )
    own.start()

    def turn(a, p):
        lo = pltpu.roll(a, 1, 1)
        hi = pltpu.roll(a, wide - 1, 1)
        stacked = jnp.concatenate([lo, a, hi, jnp.zeros((kq - 3 * cp, wide), F32)], axis=0)
        xs[p] = stacked.astype(BF16).T

    def turn_row(r, carry):
        turn(raw_row(r), r + 2)
        return carry

    lax.fori_loop(0, rows, turn_row, 0, unroll=4)

    for load in loads[1:]:
        load.wait()
    for a in range(3):
        pieces = []
        for j in range(3):
            pieces.append(w1[3 * a + j].astype(F32))
            if cp > chans:
                pieces.append(jnp.zeros((cp - chans, hid), F32))
        pieces.append(jnp.zeros((kq - 3 * cp, hid), F32))
        w1s[pl.ds(a * kq, kq), :] = (0.5 * jnp.concatenate(pieces, axis=0)).astype(BF16)

    def turn_weight(tap, carry):
        w2s[pl.ds(pl.multiple_of(tap * hid, hid), hid), :] = w2[tap].T
        return carry

    lax.fori_loop(0, 9, turn_weight, 0)

    each(lambda copy: copy.wait_recv(), 2)
    lax.fori_loop(cut1, n - 1, field_start, 0)
    tall = rows + 4
    step = en.shape[1]
    for side, p in ((0, 0), (1, rows + 2)):
        for j in range(2):
            turn(rrecv[side, j].astype(F32)[0:cp], p + j)

    lane = lax.broadcasted_iota(jnp.int32, (1, kq), 1)
    for side in range(2):
        far = jnp.concatenate([krecv[2 * side], hcol[side].astype(F32), krecv[2 * side + 1]], axis=0)
        mine = jnp.concatenate(
            [
                xs[p, (wide - 16 if side == 0 else 0) : (wide if side == 0 else 16), :].astype(F32)[(15 if side == 0 else 0) : (16 if side == 0 else 1)]
                for p in (0, 1)
            ]
            + [cols[1 - side]]
            + [
                xs[p, (wide - 16 if side == 0 else 0) : (wide if side == 0 else 16), :].astype(F32)[(15 if side == 0 else 0) : (16 if side == 0 else 1)]
                for p in (rows + 2, rows + 3)
            ],
            axis=0,
        )
        theirs = lane < 2 * cp if side == 0 else lane >= cp
        en[side, 0:tall, :] = jnp.where(theirs, far, mine)
        en[2 + side, 0:tall, :] = pltpu.roll(far, kq - cp if side == 0 else cp, 1)

    def patch(p, carry):
        first = xs[p, 0:16, :].astype(F32)
        spot = lax.broadcasted_iota(jnp.int32, (16, 1), 0)
        xs[p, 0:16, :] = jnp.where((spot == 0) & (lane < cp), en[2, pl.ds(p, 1), :], first).astype(BF16)
        last = xs[p, wide - 16 : wide, :].astype(F32)
        xs[p, wide - 16 : wide, :] = jnp.where(
            (spot == 15) & (lane >= 2 * cp) & (lane < 3 * cp), en[3, pl.ds(p, 1), :], last
        ).astype(BF16)
        return carry

    lax.fori_loop(0, tall, patch, 0)

    many = pltpu.make_async_copy(stats.at[pl.ds(0, n - 1)], stats.at[pl.ds(0, n - 1)], st_recv)
    many.wait()
    sums = jnp.sum(stats[...], axis=0)
    cells = n * rows * wide
    mean = sums[0:1] / cells
    scale = 1.0 / jnp.sqrt(sums[1:2] / cells - mean * mean + 1e-05)

    def thrice(v):
        v = v[:, 0:cp]
        return jnp.concatenate([v, v, v, jnp.zeros((1, kq - 3 * cp), F32)], axis=1)

    mean3 = thrice(mean)
    scale3 = thrice(scale)

    def normal(p, carry):
        xn[p] = ((xs[p].astype(F32) - mean3) * scale3).astype(BF16)
        return carry

    lax.fori_loop(0, tall, normal, 0, unroll=2)

    @pl.when(lat == 0)
    def _():
        xn[0:2] = jnp.zeros((2, wide, kq), BF16)

    @pl.when(lat == n_lat - 1)
    def _():
        xn[rows + 2 : rows + 4] = jnp.zeros((2, wide, kq), BF16)

    first = jnp.where(lat == 0, 0, -2)
    last = jnp.where(lat == n_lat - 1, rows - 1, rows + 1)
    line = lax.broadcasted_iota(jnp.int32, (step, 1), 0) - 2
    inside = (line >= first) & (line <= last)
    bias1 = 0.5 * b1[...]
    bias2 = b2[...]
    edge = jnp.concatenate(
        [jnp.where(inside, (en[side] - mean3) * scale3, 0.0) for side in range(2)], axis=0
    ).astype(BF16)
    z = [jnp.dot(edge, w1s[pl.ds(a * kq, kq), :], preferred_element_type=F32) for a in range(3)]
    for side in range(2):
        at = side * step
        h = z[0][at : at + rows + 2] + z[1][at + 1 : at + rows + 3] + z[2][at + 2 : at + rows + 4] + bias1
        eh[side, pl.ds(0, rows + 2), :] = twice_half_gelu(h)

    def conv1(q, g):
        left = jnp.concatenate([xn[pl.ds(q + a, g)].reshape(g * wide, kq) for a in range(3)], axis=1)
        acc1[0 : g * wide] = jnp.dot(left, w1s[...], preferred_element_type=F32)

    def store1(q, g):
        for k in range(g):
            hp[k, 8 : 8 + wide, :] = twice_half_gelu(acc1[k * wide : (k + 1) * wide, :] + bias1)
            hp[k, 7:8, :] = eh[0, pl.ds(q + k, 1), :]
            hp[k, 8 + wide : 9 + wide, :] = eh[1, pl.ds(q + k, 1), :]
            for m in range(3):
                hs[q + k, :, m * hid : (m + 1) * hid] = hp[k, 7 + m : 7 + m + wide, :].astype(BF16)

    def phase1(b, carry):
        store1(G1 * (b - 1), G1)
        conv1(G1 * b, G1)
        return carry

    conv1(0, G1)
    whole1 = (rows + 2) // G1
    lax.fori_loop(1, whole1, phase1, 0)
    store1(G1 * (whole1 - 1), G1)
    if (rows + 2) % G1:
        conv1(G1 * whole1, (rows + 2) % G1)
        store1(G1 * whole1, (rows + 2) % G1)

    @pl.when(lat == 0)
    def _():
        hs[0] = jnp.zeros((wide, 3 * hid), BF16)

    @pl.when(lat == n_lat - 1)
    def _():
        hs[rows + 1] = jnp.zeros((wide, 3 * hid), BF16)

    def conv2(q):
        left = jnp.concatenate([hs[pl.ds(q + a, G2)].reshape(G2 * wide, 3 * hid) for a in range(3)], axis=1)
        acc2[...] = jnp.dot(left, w2s[...], preferred_element_type=F32)

    def store2(q):
        for k in range(G2):
            yflat[pl.ds(q + k, hid, stride=pitch), :] = (acc2[k * wide : (k + 1) * wide, :] + bias2).T

    def phase2(b, carry):
        store2(G2 * (b - 1))
        conv2(G2 * b)
        return carry

    conv2(0)
    lax.fori_loop(1, rows // G2, phase2, 0)
    store2(rows - G2)

    chunk = hid // 8
    for k in range(8):
        part = pl.ds(k * chunk, chunk)
        feat[part] = yf[part, 0:rows, :].astype(BF16)

    own.wait()
    others = moved.at[pl.ds(0, (n - 1) * slots)]
    pltpu.make_async_copy(others, others, mv_recv).wait()
    pltpu.make_async_copy(others, others, mv_send).wait()
    pltpu.make_async_copy(stats.at[pl.ds(0, n - 1)], stats.at[pl.ds(0, n - 1)], st_send).wait()
    each(lambda copy: copy.wait_send(), 1)


def give(chans, feat_in, moved, slot_in, feat, tile, slot, sems):
    want = pltpu.make_async_copy(slot_in, slot, sems.at[0])
    want.start()
    part = feat.shape[0] // PIECES
    for k in range(PIECES):
        piece = pl.ds(k * part, part)
        pltpu.make_async_copy(feat_in.at[piece], feat.at[piece], sems.at[1]).start()
    want.wait()

    for c in range(chans):
        pltpu.make_async_copy(moved.at[slot[c]], tile.at[c], sems.at[2]).start()
    pltpu.make_async_copy(moved.at[pl.ds(0, chans)], tile, sems.at[2]).wait()
    pltpu.make_async_copy(feat_in, feat, sems.at[1]).wait()


def body(current, next_fields, reader_slot, first_weight, first_bias, second_weight, second_bias):
    n_lat, n_lon = lax.axis_size("lat"), lax.axis_size("lon")
    n = n_lat * n_lon
    chans, rows, wide = current.shape
    slots = next_fields.shape[0]
    hid = first_weight.shape[1]
    cp = -(-chans // 8) * 8
    cb = -(-chans // 16) * 16
    kq = -(-3 * cp // LANES) * LANES
    pitch = 8 * (rows // 8 + 1 - rows // 8 % 2)
    step = -(-(rows + 4) // 16) * 16
    dims = (n_lat, n_lon, chans, rows, wide, slots, hid)
    vmem = pl.BlockSpec(memory_space=pltpu.VMEM)
    hbm = pl.BlockSpec(memory_space=pltpu.HBM)
    hold = pltpu.with_memory_space_constraint
    made, moved = pl.pallas_call(
        functools.partial(kernel, dims),
        out_shape=(
            jax.ShapeDtypeStruct((hid, rows, wide), BF16),
            jax.ShapeDtypeStruct((n * slots, rows, wide), BF16),
        ),
        in_specs=[hbm] * 6,
        out_specs=(vmem, vmem),
        scratch_shapes=[
            pltpu.VMEM((chans, rows, wide), BF16),
            pltpu.VMEM((9, chans, hid), BF16),
            pltpu.VMEM((9, hid, hid), BF16),
            pltpu.VMEM((1, hid), F32),
            pltpu.VMEM((1, hid), F32),
            pltpu.VMEM((hid, pitch, wide), F32),
            pltpu.VMEM((cp, pitch, wide), F32),
            pltpu.VMEM((2, cp * 8, wide), F32),
            pltpu.VMEM((wide, LANES), F32),
            pltpu.VMEM((rows + 4, wide, kq), BF16),
            pltpu.VMEM((2, rows, kq), F32),
            pltpu.VMEM((2, rows, kq), BF16),
            pltpu.VMEM((2, rows, kq), BF16),
            pltpu.VMEM((4, 2, kq), F32),
            pltpu.VMEM((4, 2, kq), F32),
            pltpu.VMEM((2, 2, cb, wide), BF16),
            pltpu.VMEM((2, 2, cb, wide), BF16),
            pltpu.VMEM((4, step, kq), F32),
            pltpu.VMEM((2, step, hid), F32),
            pltpu.VMEM((rows + 4, wide, kq), BF16),
            pltpu.VMEM((G1 * wide, hid), F32),
            pltpu.VMEM((G1, wide + 16, hid), F32),
            pltpu.VMEM((rows + 2, wide, 3 * hid), BF16),
            pltpu.VMEM((G2 * wide, hid), F32),
            pltpu.VMEM((3 * kq, hid), BF16),
            pltpu.VMEM((9 * hid, hid), BF16),
            pltpu.VMEM((n, 2, LANES), F32),
            pltpu.SemaphoreType.DMA((5,)),
            pltpu.SemaphoreType.DMA,
            pltpu.SemaphoreType.DMA,
            pltpu.SemaphoreType.DMA((8,)),
            pltpu.SemaphoreType.DMA((8,)),
            pltpu.SemaphoreType.DMA,
            pltpu.SemaphoreType.DMA,
            pltpu.SemaphoreType.DMA,
        ],
        compiler_params=pltpu.CompilerParams(
            collective_id=0, has_side_effects=True, vmem_limit_bytes=40 * 1024 * 1024
        ),
    )(
        *[
            hold(x, pltpu.HBM)
            for x in (
                current, next_fields, first_weight.transpose(0, 2, 1),
                first_bias[None], second_weight, second_bias[None],
            )
        ]
    )
    return pl.pallas_call(
        functools.partial(give, chans),
        out_shape=(
            jax.ShapeDtypeStruct((hid, rows, wide), BF16),
            jax.ShapeDtypeStruct((chans, rows, wide), BF16),
        ),
        in_specs=[vmem, vmem, hbm],
        out_specs=(hbm, hbm),
        scratch_shapes=[pltpu.SMEM((chans,), jnp.int32), pltpu.SemaphoreType.DMA((3,))],
        compiler_params=pltpu.CompilerParams(vmem_limit_bytes=8 * 1024 * 1024),
    )(made, moved, hold(reader_slot, pltpu.HBM))


def solution(mesh):
    in_specs = (P(None, "lat", "lon"), P(("lat", "lon"), None, None), P(), P(), P(), P(), P())
    out_specs = (P(None, "lat", "lon"), P(None, "lat", "lon"))
    return jax.shard_map(body, mesh=mesh, in_specs=in_specs, out_specs=out_specs, check_vma=False)
```
